256 devices in a mesh: prow: 16 (over x_hi, z), pcol: 16 (over x_lo, y, core).
Axes of the slice: x: 4 (x_hi: 2, x_lo: 2; x = x_hi * 2 + x_lo), y: 4, z: 8, core: 2. Of those that a mesh axis runs over, the one named last changes fastest.
Arguments:
- system: bfloat16 [12288, 65536], P('prow', 'pcol'), may hold values from -6 to 6
- row_outer: float32 [12288], P('prow'), may hold values from 0.5 to 2
- row_inner: float32 [12288], P('prow'), may hold values from 0.5 to 2
- col_outer: float32 [65536], P('pcol'), may hold values from 0.5 to 2
- col_inner: float32 [65536], P('pcol'), may hold values from 0.5 to 2
- diag_inverse: bfloat16 [512, 512], replicated, may hold values from -0.01171875 to 0.01171875
Outputs:
- trailing: bfloat16 [12288, 65536], P('prow', 'pcol')
The draws below stay inside these ranges and needn't reach their ends.
All inputs are finite; a program needn't handle non-finite values.
Results may differ from the reference program's by a relative error of at most 0.0089.
Values may be sent and summed in bfloat16 or wider, within the bound.
No kernel may reach another device: no remote copies, remote signals or barrier semaphores. Data moves between devices by JAX's collectives and lax.ppermute only.
A program may use at most 192 MiB of HBM per device.

```python
import math
import jax
import jax.numpy as jnp

N = 65536
PANEL = 512
M = 12288


def level_of(own_key, shape, pieces, low, largest):
    factor_of = 1.0
    for dim, parts in pieces:
        draws = jax.random.uniform(jax.random.fold_in(jax.random.fold_in(own_key, 6), dim), (parts,), jnp.float32, low / len(pieces), largest / len(pieces))
        factor_of = factor_of * jnp.repeat(jnp.exp(draws), shape[dim] // parts).reshape((-1,) + (1,) * (len(shape) - 1 - dim))
    return factor_of


def normal_values(key, extent, spread, bound, split=(), held_as=jnp.bfloat16):
    result = spread * jax.random.normal(key, extent, jnp.float32)
    if split:
        result = result * level_of(key, extent, split, -0.22, 0.18)
    return jnp.clip(result, -bound, bound).astype(held_as)


def setup_inputs(seed: int = 0) -> dict:
    splits = jax.random.split(jax.random.key(seed), 7)
    system = normal_values(splits[0], (M, N), 1.0, 6.0, ((0, 16), (1, 16)))
    row_outer = jnp.clip(jnp.exp(math.log(2.0) - 1.3862944 * jax.random.uniform(splits[1], (M,), jnp.float32) ** level_of(splits[1], (M,), ((0, 16),), -0.2, 0.2)), 0.5, 2.0)
    row_inner = jnp.clip(jnp.exp(math.log(2.0) - 1.3862944 * jax.random.uniform(splits[2], (M,), jnp.float32) ** level_of(splits[2], (M,), ((0, 16),), -0.2, 0.2)), 0.5, 2.0)
    col_outer = jnp.clip(jnp.exp(math.log(2.0) - 1.3862944 * jax.random.uniform(splits[3], (N,), jnp.float32) ** level_of(splits[3], (N,), ((0, 16),), -0.2, 0.2)), 0.5, 2.0)
    col_inner = jnp.clip(jnp.exp(math.log(2.0) - 1.3862944 * jax.random.uniform(splits[4], (N,), jnp.float32) ** level_of(splits[4], (N,), ((0, 16),), -0.2, 0.2)), 0.5, 2.0)
    diag_inverse = normal_values(splits[5], (PANEL, PANEL), (PANEL * PANEL) ** -0.5, 0.01171875)
    return dict(system=system, row_outer=row_outer, row_inner=row_inner, col_outer=col_outer, col_inner=col_inner, diag_inverse=diag_inverse)


root_half = 0.7071067811865476


def mix_rows(values, weights, half):
    rows, cols = values.shape
    blocks = values.astype(jnp.float32).reshape(rows // (2 * half), 2, half, cols)
    scales = weights.reshape(rows // (2 * half), 2, half, 1)
    upper = scales[:, 0] * (blocks[:, 0] + blocks[:, 1]) * root_half
    lower = scales[:, 1] * (blocks[:, 0] - blocks[:, 1]) * root_half
    return jnp.stack([upper, lower], axis=1).reshape(rows, cols).astype(jnp.bfloat16)


def mix_cols(values, weights, half):
    rows, cols = values.shape
    blocks = values.astype(jnp.float32).reshape(rows, cols // (2 * half), 2, half)
    scales = weights.reshape(1, cols // (2 * half), 2, half)
    upper = scales[:, :, 0] * (blocks[:, :, 0] + blocks[:, :, 1]) * root_half
    lower = scales[:, :, 1] * (blocks[:, :, 0] - blocks[:, :, 1]) * root_half
    return jnp.stack([upper, lower], axis=2).reshape(rows, cols).astype(jnp.bfloat16)


def reference(system, row_outer, row_inner, col_outer, col_inner, diag_inverse):
    first = mix_rows(system, row_outer, M // 2)
    second = mix_rows(first, row_inner, M // 4)
    third = mix_cols(second, col_outer, N // 2)
    transformed = mix_cols(third, col_inner, N // 4)
    left = jnp.dot(transformed[:, :PANEL], diag_inverse, preferred_element_type=jnp.float32).astype(jnp.bfloat16)
    update = jnp.dot(left, transformed[:PANEL, :], preferred_element_type=jnp.float32)
    return (transformed.astype(jnp.float32) - update).astype(jnp.bfloat16)
```

```python
import functools
import jax
import jax.numpy as jnp
from jax import lax
from jax.experimental import pallas as pl
from jax.experimental.pallas import tpu as pltpu
from jax.sharding import Mesh, PartitionSpec as P

root_half = 0.7071067811865476
f32, bf16 = jnp.float32, jnp.bfloat16
X4 = ("xh", "xl")
Y4 = ("yh", "yl")


def rows_of(total):
    for tile in (192, 96, 64, 48, 32, 16, 8):
        if total % tile == 0:
            return tile
    return total


def sub_rows(tile):
    return 16 if tile % 16 == 0 else 8


def call(body, grid, ins, outs, shapes, flops, nbytes, aliases=None, name=None):
    return pl.pallas_call(
        body,
        grid_spec=pltpu.PrefetchScalarGridSpec(
            num_scalar_prefetch=1, grid=grid, in_specs=ins, out_specs=outs
        ),
        out_shape=shapes,
        input_output_aliases=aliases or {},
        cost_estimate=pl.CostEstimate(flops=flops, bytes_accessed=nbytes, transcendentals=0),
        compiler_params=pltpu.CompilerParams(vmem_limit_bytes=8 * 1024 * 1024),
        name=name,
    )


def split_body(n, s, *refs):
    ins, outs = refs[:6], refs[6:]
    for e in range(3):
        outs[e][0] = ins[e][...]
        outs[e][1] = ins[3 + e][...]


def split_slices(scalars, system, other, width):
    rows = system.shape[0]
    tile = rows_of(rows)
    own = [pl.BlockSpec((tile, width), lambda i, s, e=e: (i, s[4 + e])) for e in (1, 2, 3)]
    got = [pl.BlockSpec((tile, width), lambda i, s, e=e: (i, s[e])) for e in (1, 2, 3)]
    out = [pl.BlockSpec((2, tile, width), lambda i, s: (0, i, 0))] * 3
    shape = [jax.ShapeDtypeStruct((2, rows, width), bf16)] * 3
    size = 3 * 2 * rows * width
    return call(functools.partial(split_body, 0), (rows // tile,), own + got, out, shape, size, 4 * size, name="split")(
        scalars, *([system] * 3), *([other] * 3)
    )


def rounded(v):
    return v.astype(bf16).astype(f32)


def mix_body(step, s, own, got, r1, r2, r3, wrow, wcol, out):
    count = own.shape[0] // step

    @pl.loop(0, count)
    def _(t):
        at = pl.ds(pl.multiple_of(t * step, step), step)
        w = wrow[at, :]
        lows, highs = [], []
        for ez in range(2):
            mine = (own if ez == 0 else got)[at, :].astype(f32)
            p = [[mine, r1[ez, at, :].astype(f32)], [r2[ez, at, :].astype(f32), r3[ez, at, :].astype(f32)]]
            lows.append([rounded((p[0][el] + p[1][el]) * w[:, ez : ez + 1]) for el in range(2)])
            highs.append([rounded((p[0][el] - p[1][el]) * w[:, 2 + ez : 3 + ez]) for el in range(2)])
        for xh, f in enumerate((lows, highs)):
            for zh in range(2):
                scale = w[:, 4 + 2 * xh + zh : 5 + 2 * xh + zh]
                g = [rounded((f[0][el] + f[1][el] if zh == 0 else f[0][el] - f[1][el]) * scale) for el in range(2)]
                out[2 * xh, zh, at, :] = ((g[0] + g[1]) * wcol[0:1, :]).astype(bf16)
                out[2 * xh + 1, zh, at, :] = ((g[0] - g[1]) * wcol[1:2, :]).astype(bf16)


def mix(scalars, system, other, received, wrow, wcol):
    rows = system.shape[0]
    width = wcol.shape[1]
    tile = rows_of(rows)
    ins = [
        pl.BlockSpec((tile, width), lambda i, s: (i, s[4])),
        pl.BlockSpec((tile, width), lambda i, s: (i, s[0])),
        *[pl.BlockSpec((2, tile, width), lambda i, s: (0, i, 0))] * 3,
        pl.BlockSpec((tile, 8), lambda i, s: (i, 0)),
        pl.BlockSpec((8, width), lambda i, s: (0, 0)),
    ]
    out = pl.BlockSpec((4, 2, tile, width), lambda i, s: (0, 0, i, 0))
    shape = jax.ShapeDtypeStruct((4, 2, rows, width), bf16)
    size = 8 * rows * width
    return call(
        functools.partial(mix_body, sub_rows(tile)), (rows // tile,), ins, out, shape, 8 * size, 4 * size, name="mix"
    )(scalars, system, other, *received, wrow, wcol)


def inner_body(step, s, mine, partner, wcol, out):
    count = mine.shape[2] // step

    @pl.loop(0, count)
    def _(t):
        at = pl.ds(pl.multiple_of(t * step, step), step)
        for x in range(4):
            for zh in range(2):
                v = mine[x, zh, at, :].astype(f32) * wcol[4:5, :] + partner[x, zh, at, :].astype(f32)
                out[x, zh, at, :] = (v * wcol[2 + x % 2 : 3 + x % 2, :]).astype(bf16)


def inner(scalars, mine, partner, wcol):
    _, _, rows, width = mine.shape
    tile = rows_of(rows)
    big = pl.BlockSpec((4, 2, tile, width), lambda i, s: (0, 0, i, 0))
    size = 8 * rows * width
    return call(
        functools.partial(inner_body, sub_rows(tile)),
        (rows // tile,),
        [big, big, pl.BlockSpec((8, width), lambda i, s: (0, 0))],
        big,
        jax.ShapeDtypeStruct(mine.shape, bf16),
        4 * size,
        6 * size,
        name="inner",
    )(scalars, mine, partner, wcol)


def factor_body(s, p0, p1, p2, p3, dinv, out):
    width = p0.shape[-1]
    for a in range(2):
        for b in range(2):
            acc = None
            for e, p in enumerate((p0, p1, p2, p3)):
                at = pl.ds(pl.multiple_of(s[e] * width, width), width)
                d = jnp.dot(p[a, b], dinv[at, :], preferred_element_type=f32)
                acc = d if acc is None else acc + d
            out[a, b] = acc.astype(bf16)


def factor(scalars, pieces, dinv):
    _, _, rows, width = pieces[0].shape
    panel = dinv.shape[0]
    tile = rows_of(rows)
    return call(
        factor_body,
        (rows // tile,),
        [pl.BlockSpec((2, 2, tile, width), lambda i, s: (0, 0, i, 0))] * 4
        + [pl.BlockSpec((panel, panel), lambda i, s: (0, 0))],
        pl.BlockSpec((2, 2, tile, panel), lambda i, s: (0, 0, i, 0)),
        jax.ShapeDtypeStruct((2, 2, rows, panel), bf16),
        8 * rows * panel * panel,
        16 * rows * panel,
        name="factor",
    )(scalars, *pieces, dinv)


def update_body(s, full, left, top, *outs):
    for e in range(4):
        x = s[e]
        for zh in range(2):
            d = jnp.dot(left[x // 2, zh], top[x % 2], preferred_element_type=f32)
            outs[e][zh] = (full[x, zh].astype(f32) - d).astype(bf16)


def update(scalars, full, left, top):
    _, _, rows, width = full.shape
    panel = left.shape[-1]
    tile = rows_of(rows)
    out = pl.BlockSpec((2, tile, width), lambda i, s: (0, i, 0))
    size = 8 * rows * width
    return call(
        update_body,
        (rows // tile,),
        [
            pl.BlockSpec((4, 2, tile, width), lambda i, s: (0, 0, i, 0)),
            pl.BlockSpec((2, 2, tile, panel), lambda i, s: (0, 0, i, 0)),
            pl.BlockSpec((2, panel, width), lambda i, s: (0, 0, 0)),
        ],
        [out] * 4,
        [jax.ShapeDtypeStruct((2, rows, width), bf16)] * 4,
        2 * size * panel,
        4 * size + 8 * rows * panel,
        name="update",
    )(scalars, full, left, top)


def gather_body(s, p0, p1, p2, p3, keep, send):
    width = p0.shape[-1]
    zh = s[8]
    for e, p in enumerate((p0, p1, p2, p3)):
        at = pl.ds(pl.multiple_of(s[e] * width, width), width)
        keep[:, at] = p[zh]
        send[:, at] = p[1 - zh]


def gather_slices(scalars, pieces):
    _, rows, width = pieces[0].shape
    tile = rows_of(rows)
    out = pl.BlockSpec((tile, 4 * width), lambda i, s: (i, 0))
    size = 8 * rows * width
    return call(
        gather_body,
        (rows // tile,),
        [pl.BlockSpec((2, tile, width), lambda i, s: (0, i, 0))] * 4,
        [out] * 2,
        [jax.ShapeDtypeStruct((rows, 4 * width), bf16)] * 2,
        size,
        4 * size,
        name="gather",
    )(scalars, *pieces)


def place_body(s, keep, got, *refs):
    out = refs[-1]
    half = keep.shape[1]
    zh = s[8]
    out[:, pl.ds(pl.multiple_of(zh * half, half), half)] = keep[...]
    out[:, pl.ds(pl.multiple_of((1 - zh) * half, half), half)] = got[...]


def place(scalars, keep, got, whole, k, columns):
    rows, half = keep.shape
    tile = rows_of(rows)
    piece = pl.BlockSpec((tile, half), lambda i, s: (i, 0))
    ins, args, aliases = [piece, piece], [keep, got], {}
    if whole is not None:
        ins.append(pl.BlockSpec(memory_space=pl.ANY))
        args.append(whole)
        aliases = {3: 0}
    return call(
        place_body,
        (rows // tile,),
        ins,
        pl.BlockSpec((tile, 2 * half), lambda i, s: (i, k)),
        jax.ShapeDtypeStruct((rows, columns), bf16),
        rows * half,
        8 * rows * half,
        aliases,
        name="place",
    )(scalars, *args)


def flip(x, axis):
    return lax.ppermute(x, axis, [(0, 1), (1, 0)])


def flip_x(x, e):
    return lax.ppermute(x, X4, [(i, i ^ e) for i in range(4)])


def per_device(system, row_outer, row_inner, col_outer, col_inner, diag_inverse):
    rows, cols = system.shape
    panel = diag_inverse.shape[0]
    half = panel
    width = half // 4
    chunks = cols // (2 * half)
    xh, xl = lax.axis_index("xh"), lax.axis_index("xl")
    zh, zl = lax.axis_index("zh"), lax.axis_index("zl")
    yh = lax.axis_index("yh")
    y, core = lax.axis_index(Y4), lax.axis_index("core")
    x = 2 * xh + xl
    order = [x ^ e for e in range(4)]
    scalars = [
        jnp.stack(order + [(2 * k + zh) * 4 + o for o in order] + [zh, x]).astype(jnp.int32) for k in range(chunks)
    ]

    def half_of(k, which):
        return lax.dynamic_slice(system, (0, (2 * k + which) * half), (rows, half))

    other = [flip(half_of(k, 1 - zh), "zh") for k in range(chunks)]

    sign_x = (1 - 2 * xh).astype(f32)
    sign_l = (1 - 2 * xl).astype(f32)
    sign_z = (1 - 2 * zh).astype(f32)
    sign_y = (1 - 2 * yh).astype(f32)
    wr = lax.all_gather(jnp.stack([row_outer, row_inner]), ("xh", "zh")).reshape(2, 2, 2, rows) * root_half
    outer, inn = wr[:, :, 0], wr[:, :, 1]
    outer = jnp.where(zh == 0, outer, outer[:, ::-1])
    wrow = jnp.stack(
        [outer[0, 0], outer[0, 1], outer[1, 0] * sign_x, outer[1, 1] * sign_x]
        + [inn[0, 0], inn[0, 1] * sign_z, inn[1, 0], inn[1, 1] * sign_z],
        axis=1,
    )
    wc = lax.all_gather(jnp.stack([col_outer, col_inner]), "xl").reshape(2, 2, chunks, 2, 4, width) * root_half
    wc = lax.dynamic_index_in_dim(wc, zh, 3, keepdims=False)
    wc = lax.dynamic_index_in_dim(wc, x, 3, keepdims=False)
    ones = jnp.ones((width,), f32)
    wcol = [
        jnp.stack(
            [wc[0, 0, k], wc[1, 0, k] * sign_l, wc[0, 1, k], wc[1, 1, k], ones * sign_y, ones, ones, ones]
        )
        for k in range(chunks)
    ]

    left = None
    whole = None
    for k in range(chunks):
        s = scalars[k]
        pieces = split_slices(s, system, other[k], width)
        received = [flip_x(p, e + 1) for e, p in enumerate(pieces)]
        mixed = mix(s, system, other[k], received, wrow, wcol[k])
        full = inner(s, mixed, flip(mixed, "yh"), wcol[k])
        own = full[0:2, 0, :panel]
        hop1 = lax.ppermute(own, "zl", [(0, 1)])
        hop2 = lax.ppermute(hop1, "zl", [(1, 2)])
        hop3 = lax.ppermute(hop2, "zl", [(2, 3)])
        top = jnp.where(zl == 0, own, hop1 + hop2 + hop3)
        if k == 0:
            lead = full[0::2]
            lead = jnp.where(zh == 0, lead, lax.ppermute(lead, "zh", [(0, 1)]))
            up = lax.ppermute(lead, Y4, [(0, 1)])
            down = lax.ppermute(lead, Y4, [(0, 3)])
            far = lax.ppermute(up, Y4, [(1, 2)])
            lead = jnp.where(y == 0, lead, up + down + far)
            lead = jnp.where(core == 0, lead, lax.ppermute(lead, "core", [(0, 1)]))
            left = factor(s, [lead] + [flip_x(lead, e) for e in (1, 2, 3)], diag_inverse)
        done = update(s, full, left, top)
        back = [done[0]] + [flip_x(done[e], e) for e in (1, 2, 3)]
        keep, send = gather_slices(s, back)
        whole = place(s, keep, flip(send, "zh"), whole, k, cols)
    return whole


def solution(mesh):
    fine = Mesh(
        mesh.devices.reshape(2, 2, 4, 2, 2, 2, 2), ("xh", "zh", "zl", "xl", "yh", "yl", "core")
    )
    prow, pcol = ("xh", "zh", "zl"), ("xl", "yh", "yl", "core")
    in_specs = (P(prow, pcol), P(prow), P(prow), P(pcol), P(pcol), P())
    return jax.shard_map(
        per_device, mesh=fine, in_specs=in_specs, out_specs=P(prow, pcol), check_vma=False
    )
```

```python
import functools
import jax
import jax.numpy as jnp
from jax import lax
from jax.experimental import pallas as pl
from jax.experimental.pallas import tpu as pltpu
from jax.sharding import Mesh, PartitionSpec as P

root_half = 0.7071067811865476
f32, bf16 = jnp.float32, jnp.bfloat16
X4 = ("xh", "xl")
COLS = ("xl", "yh", "yl", "core")


def rows_of(total):
    for tile in (192, 96, 64, 48, 32, 16, 8):
        if total % tile == 0:
            return tile
    return total


def small_rows_of(total):
    tile = rows_of(total)
    return tile // 2 if tile % 32 == 0 else tile


def sub_rows(tile):
    return 16 if tile % 16 == 0 else 8


def call(body, grid, ins, outs, shapes, flops, nbytes, aliases=None):
    return pl.pallas_call(
        body,
        grid=grid,
        in_specs=ins,
        out_specs=outs,
        out_shape=shapes,
        input_output_aliases=aliases or {},
        cost_estimate=pl.CostEstimate(flops=flops, bytes_accessed=nbytes, transcendentals=0),
        compiler_params=pltpu.CompilerParams(vmem_limit_bytes=8 * 1024 * 1024),
    )


def split_body(z, mine, other, out):
    zh = z[0]
    width = out.shape[3]
    for j in range(4):
        at = slice(j * width, (j + 1) * width)
        out[j, zh] = mine[:, at]
        out[j, 1 - zh] = other[:, at]


def split_slots(z, mine, other):
    rows, half = mine.shape
    tile = rows_of(rows)
    width = half // 4
    size = 8 * rows * width
    block = pl.BlockSpec((tile, half), lambda i: (i, 0))
    return call(
        split_body,
        (rows // tile,),
        [pl.BlockSpec(memory_space=pltpu.SMEM), block, block],
        pl.BlockSpec((4, 2, tile, width), lambda i: (0, 0, i, 0)),
        jax.ShapeDtypeStruct((4, 2, rows, width), bf16),
        size,
        4 * size,
    )(z, mine, other)


def rounded(v):
    return v.astype(bf16).astype(f32)


def mix_body(step, blocks, wrow, wcol, out):
    count = blocks.shape[2] // step

    @pl.loop(0, count, unroll=2 if count % 2 == 0 else 1)
    def _(t):
        at = pl.ds(pl.multiple_of(t * step, step), step)
        w = wrow[at, :]
        p = [blocks[j % 4, j // 4, at, :].astype(f32) for j in range(8)]
        first = {}
        for zh in range(2):
            for xl in range(2):
                a, b = p[4 * zh + xl], p[4 * zh + 2 + xl]
                first[0, zh, xl] = rounded((a + b) * w[:, zh : zh + 1])
                first[1, zh, xl] = rounded((a - b) * w[:, 2 + zh : 3 + zh])
        for xh in range(2):
            for zh in range(2):
                scale = w[:, 4 + 2 * xh + zh : 5 + 2 * xh + zh]
                g = []
                for xl in range(2):
                    a, b = first[xh, 0, xl], first[xh, 1, xl]
                    g.append(rounded((a + b if zh == 0 else a - b) * scale))
                out[2 * xh, zh, at, :] = ((g[0] + g[1]) * wcol[0:1, :]).astype(bf16)
                out[2 * xh + 1, zh, at, :] = ((g[0] - g[1]) * wcol[1:2, :]).astype(bf16)


def mix(blocks, wrow, wcol, k):
    _, _, rows, width = blocks.shape
    tile = rows_of(rows)
    big = pl.BlockSpec((4, 2, tile, width), lambda i: (0, 0, i, 0))
    size = 8 * rows * width
    return call(
        functools.partial(mix_body, sub_rows(tile)),
        (rows // tile,),
        [big, pl.BlockSpec((tile, 8), lambda i: (i, 0)), pl.BlockSpec((None, 8, width), lambda i: (k, 0, 0))],
        big,
        jax.ShapeDtypeStruct(blocks.shape, bf16),
        8 * size,
        4 * size,
    )(blocks, wrow, wcol)


def inner_body(step, mine, partner, wcol, out):
    count = mine.shape[2] // step

    @pl.loop(0, count, unroll=2 if count % 2 == 0 else 1)
    def _(t):
        at = pl.ds(pl.multiple_of(t * step, step), step)
        for j in range(4):
            for zh in range(2):
                v = mine[j, zh, at, :].astype(f32) * wcol[4:5, :] + partner[j, zh, at, :].astype(f32)
                out[j, zh, at, :] = (v * wcol[2 + j % 2 : 3 + j % 2, :]).astype(bf16)


def inner(mine, partner, wcol, k):
    _, _, rows, width = mine.shape
    tile = rows_of(rows)
    big = pl.BlockSpec((4, 2, tile, width), lambda i: (0, 0, i, 0))
    size = 8 * rows * width
    return call(
        functools.partial(inner_body, sub_rows(tile)),
        (rows // tile,),
        [big, big, pl.BlockSpec((None, 8, width), lambda i: (k, 0, 0))],
        big,
        jax.ShapeDtypeStruct(mine.shape, bf16),
        4 * size,
        6 * size,
    )(mine, partner, wcol)


def factor_body(step, p0, p1, p2, p3, wrow, out):
    count = wrow.shape[0] // step

    @pl.loop(0, count)
    def _(t):
        at = pl.ds(pl.multiple_of(t * step, step), step)
        w = wrow[at, :]
        p = [v[at, :].astype(f32) for v in (p0, p1, p2, p3)]
        for xh in range(2):
            f = []
            for ez in range(2):
                v = p[ez] + p[2 + ez] if xh == 0 else p[ez] - p[2 + ez]
                f.append(v * w[:, 2 * xh + ez : 2 * xh + ez + 1])
            for zh in range(2):
                v = f[0] + f[1] if zh == 0 else f[0] - f[1]
                out[xh, zh, at, :] = (v * w[:, 4 + 2 * xh + zh : 5 + 2 * xh + zh]).astype(bf16)


def factor(pieces, wrow):
    rows, panel = pieces[0].shape
    tile = small_rows_of(rows)
    size = 4 * rows * panel
    return call(
        functools.partial(factor_body, sub_rows(tile)),
        (rows // tile,),
        [pl.BlockSpec((tile, panel), lambda i: (i, 0))] * 4 + [pl.BlockSpec((tile, 8), lambda i: (i, 0))],
        pl.BlockSpec((2, 2, tile, panel), lambda i: (0, 0, i, 0)),
        jax.ShapeDtypeStruct((2, 2, rows, panel), bf16),
        5 * size,
        4 * size,
    )(*pieces, wrow)


def update_body(place, full, mine, passed_left, own, hop1, hop2, hop3, out, top):
    width = full.shape[3]

    @pl.when(pl.program_id(0) == 0)
    def _():
        passed = hop1[...] + hop2[...] + hop3[...]
        top[...] = jnp.where(place[0] == 0, own[...], passed)

    for zh in range(2):
        for xh in range(2):
            left = jnp.where(place[1] == 0, mine[xh, zh], passed_left[xh, zh])
            d = jnp.dot(left, top[...], preferred_element_type=f32)
            for xl in range(2):
                j = 2 * xh + xl
                out[j, zh] = (full[j, zh].astype(f32) - d[:, xl * width : (xl + 1) * width]).astype(bf16)


def update(place, full, left, tops):
    _, _, rows, width = full.shape
    panel = left[0].shape[-1]
    tile = small_rows_of(rows)
    big = pl.BlockSpec((4, 2, tile, width), lambda i: (0, 0, i, 0))
    size = 8 * rows * width
    return pl.pallas_call(
        update_body,
        grid=(rows // tile,),
        in_specs=[
            pl.BlockSpec(memory_space=pltpu.SMEM),
            big,
            *[pl.BlockSpec((2, 2, tile, panel), lambda i: (0, 0, i, 0))] * 2,
            *[pl.BlockSpec((panel, 2 * width), lambda i: (0, 0))] * 4,
        ],
        out_specs=big,
        out_shape=jax.ShapeDtypeStruct(full.shape, bf16),
        scratch_shapes=[pltpu.VMEM((panel, 2 * width), bf16)],
        cost_estimate=pl.CostEstimate(
            flops=2 * size * panel, bytes_accessed=4 * size + 8 * rows * panel, transcendentals=0
        ),
        compiler_params=pltpu.CompilerParams(vmem_limit_bytes=8 * 1024 * 1024),
        name="update",
    )(place, full, *left, *tops)


def gather_body(z, slots, keep, away):
    zh = z[0]
    width = slots.shape[3]
    for j in range(4):
        at = slice(j * width, (j + 1) * width)
        keep[:, at] = slots[j, zh]
        away[:, at] = slots[j, 1 - zh]


def gather_slots(z, slots):
    _, _, rows, width = slots.shape
    tile = rows_of(rows)
    out = pl.BlockSpec((tile, 4 * width), lambda i: (i, 0))
    size = 8 * rows * width
    return call(
        gather_body,
        (rows // tile,),
        [pl.BlockSpec(memory_space=pltpu.SMEM), pl.BlockSpec((4, 2, tile, width), lambda i: (0, 0, i, 0))],
        [out] * 2,
        [jax.ShapeDtypeStruct((rows, 4 * width), bf16)] * 2,
        size,
        4 * size,
    )(z, slots)


def place_body(z, keep, got, *refs):
    out = refs[-1]
    half = keep.shape[1]
    zh = z[0]
    out[:, pl.ds(pl.multiple_of(zh * half, half), half)] = keep[...]
    out[:, pl.ds(pl.multiple_of((1 - zh) * half, half), half)] = got[...]


def place(z, keep, got, whole, k, columns):
    rows, half = keep.shape
    tile = rows_of(rows)
    piece = pl.BlockSpec((tile, half), lambda i: (i, 0))
    ins, args, aliases = [pl.BlockSpec(memory_space=pltpu.SMEM), piece, piece], [z, keep, got], {}
    if whole is not None:
        ins.append(pl.BlockSpec(memory_space=pl.ANY))
        args.append(whole)
        aliases = {3: 0}
    return call(
        place_body,
        (rows // tile,),
        ins,
        pl.BlockSpec((tile, 2 * half), lambda i: (i, k)),
        jax.ShapeDtypeStruct((rows, columns), bf16),
        rows * half,
        8 * rows * half,
        aliases,
    )(*args)


def flip(x, axis):
    return lax.ppermute(x, axis, [(0, 1), (1, 0)])


def trade(x):
    return lax.all_to_all(x, X4, 0, 0, tiled=True)


def steps(system, row_outer, row_inner, col_outer, col_inner, diag_inverse):
    rows, cols = system.shape
    panel = diag_inverse.shape[0]
    width = panel // 4
    chunks = cols // (8 * width)
    xh, xl = lax.axis_index("xh"), lax.axis_index("xl")
    zh, zl = lax.axis_index("zh"), lax.axis_index("zl")
    yh = lax.axis_index("yh")
    y, core = 2 * yh + lax.axis_index("yl"), lax.axis_index("core")

    wr = jnp.stack([row_outer, row_inner]) * root_half
    wr = jnp.stack([wr, flip(wr, "zh")])
    half = 4 * width
    z = zh.reshape(1)
    halves = lambda k, which: lax.dynamic_slice(system, (0, (2 * k + which) * half), (rows, half))
    arrived = []
    for k in range(chunks):
        other = flip(halves(k, 1 - zh), "zh")
        slots = split_slots(z, halves(k, zh), other)
        arrived.append(trade(slots))

    sign_x = (1 - 2 * xh).astype(f32)
    sign_z = (1 - 2 * zh).astype(f32)
    sign_y = (1 - 2 * yh).astype(f32)
    wx = lax.ppermute(wr, "xh", [(0, 1), (1, 0)])
    wr = jnp.stack([jnp.where(xh == 0, wr, wx), jnp.where(xh == 0, wx, wr)])
    near_outer = wr[:, :, 0]
    wr = jnp.where(zh == 0, wr, wr[:, ::-1])
    wrow = jnp.concatenate([wr[:, :, 0].reshape(4, rows), wr[:, :, 1].reshape(4, rows)]).T
    flips = jnp.stack([sign_x * 0 + 1, sign_z])
    wrel = jnp.concatenate(
        [near_outer[0], near_outer[1] * sign_x, wr[0, :, 1] * flips[:, None], wr[1, :, 1] * flips[:, None]]
    ).T
    wc = jnp.stack([col_outer, col_inner]) * root_half
    wc = wc.reshape(2, chunks, 2, 4, width)
    wc = jnp.stack([wc, flip(wc, "xl")])
    wc = jnp.where(xl == 0, wc, wc[::-1])
    wc = lax.dynamic_index_in_dim(wc, zh, 3, keepdims=False)
    wc = lax.dynamic_index_in_dim(wc, 2 * xh + xl, 3, keepdims=False)
    ones = jnp.ones((chunks, width), f32)
    wcol = jnp.stack([wc[0, 0], wc[1, 0], wc[0, 1], wc[1, 1], ones * sign_y, ones, ones, ones], axis=1)

    lead = system[:, :panel].astype(f32)
    lead = (
        (lead + lax.ppermute(system[:, :panel], COLS, [(8, 0), (12, 4)]).astype(f32)) * (col_outer[:panel] * root_half)
    ).astype(bf16)
    lead = (
        (lead.astype(f32) + lax.ppermute(lead, COLS, [(4, 0)]).astype(f32)) * (col_inner[:panel] * root_half)
    ).astype(bf16)
    lead = jnp.dot(lead, diag_inverse, preferred_element_type=f32).astype(bf16)
    near = [lax.ppermute(lead, COLS, [(0, 2 * d)]) for d in (1, 3, 2)]
    lead = jnp.where(y == 0, lead, near[0] + near[1] + near[2])
    lead = jnp.where(xl == 0, lead, lax.ppermute(lead, ("xl", "core"), [(0, 2)]))
    both = [(0, 2), (2, 0)]
    other_z = lax.ppermute(lead, ("zh", "core"), both)
    direct = [lead, other_z] + [lax.ppermute(v, ("xh", "core"), both) for v in (lead, other_z)]
    left = factor(direct, wrel)
    left = [left, flip(left, "core")]
    place_of = jnp.stack([zl, core])

    whole = None
    for k in range(chunks):
        mixed = mix(arrived[k], wrow, wcol, k)
        top = jnp.concatenate([mixed[0, 0, :panel], mixed[1, 0, :panel]], axis=1)
        top_scale = jnp.concatenate([wcol[k, 2], wcol[k, 3]])
        top = top.astype(f32) * sign_y + flip(top, "yh").astype(f32)
        top = (top * top_scale).astype(bf16)
        partner = flip(mixed, "yh")
        full = inner(mixed, partner, wcol, k)
        hops = [lax.ppermute(top, "zl", [(0, d)]) for d in (1, 2, 3)]
        done = update(place_of, full, left, [top] + hops)
        done = trade(done)
        keep, away = gather_slots(z, done)
        got = flip(away, "zh")
        whole = place(z, keep, got, whole, k, cols)
    return whole


def solution(mesh):
    fine = Mesh(
        mesh.devices.reshape(2, 2, 4, 2, 2, 2, 2), ("xh", "zh", "zl", "xl", "yh", "yl", "core")
    )
    prow, pcol = ("xh", "zh", "zl"), ("xl", "yh", "yl", "core")
    in_specs = (P(prow, pcol), P(prow), P(prow), P(pcol), P(pcol), P())
    return jax.shard_map(steps, mesh=fine, in_specs=in_specs, out_specs=P(prow, pcol), check_vma=False)
```
